32 devices in a mesh: dp: 2 (over x), ei: 4 (over z), eo: 4 (over y, core).
Axes of the slice: x: 2, y: 2, z: 4, core: 2. Of those that a mesh axis runs over, the one named last changes fastest.
Arguments:
- x: bfloat16 [131072, 1024], P(('dp', 'ei', 'eo')), parts along dimension 0
- slots: int32 [1024, 256], P(('dp', 'ei', 'eo')), parts along dimension 0
- gates: float32 [131072, 2], P(('dp', 'ei', 'eo')), parts along dimension 0
- w1: bfloat16 [32, 1024, 512], P(('ei', 'eo'))
- w3: bfloat16 [32, 1024, 512], P(('ei', 'eo'))
- w2: bfloat16 [32, 512, 1024], P(('ei', 'eo'))
- dy: bfloat16 [131072, 1024], P(('dp', 'ei', 'eo')), parts along dimension 0
Outputs:
- output 1: bfloat16 [131072, 1024], P(('dp', 'ei', 'eo')), parts along dimension 0
- output 2: bfloat16 [131072, 1024], P(('dp', 'ei', 'eo')), parts along dimension 0
- output 3: float32 [131072, 2], P(('dp', 'ei', 'eo')), parts along dimension 0
- output 4: float32 [64, 1024, 512], P(('dp', 'ei', 'eo')), parts along dimension 0
- output 5: float32 [64, 1024, 512], P(('dp', 'ei', 'eo')), parts along dimension 0
- output 6: float32 [64, 512, 1024], P(('dp', 'ei', 'eo')), parts along dimension 0
There are 2 independent parts. The reference program is written for one: setup_inputs(seed, part) draws one part's arguments, and reference() takes and returns one part's arrays. A program takes and returns all parts, laid end to end along the dimension named above; an argument that names none is the same for every part.
All inputs are finite; a program needn't handle non-finite values.
Results may differ from the reference program's by a relative error of at most 0.001.
Values are sent between devices in bfloat16 or wider.
A program may use at most 1 GiB of HBM per device.

```python
import jax
import jax.numpy as jnp
from jax import lax
import numpy as np

GROUP = 16
TOKENS = 4096
D = 1024
FF = 512
EXPERTS = 32
TOP = 2
SKEW = 1
BOUND = 256
ROWS = 64

NPER = TOKENS * TOP
NTOK = GROUP * TOKENS
NASG = GROUP * NPER
NBLK = (NASG + ROWS - 1) // ROWS + EXPERTS


def _counts():
    heavy = EXPERTS // (2 * SKEW)
    light = EXPERTS - heavy
    q, r = divmod(NPER - heavy * BOUND, light)
    return np.array([BOUND] * heavy + [q + 1] * r + [q] * (light - r), dtype=np.int64)


def setup_inputs(seed: int = 0, part: int = 0) -> dict:
    kw = jax.random.split(jax.random.key(seed), 3)
    kp = jax.random.split(jax.random.fold_in(jax.random.key(seed + 1), part), 4)
    x = jax.random.normal(kp[0], (NTOK, D), jnp.float32).astype(jnp.bfloat16)
    dy = jax.random.normal(kp[1], (NTOK, D), jnp.float32).astype(jnp.bfloat16)
    gates = jax.random.uniform(kp[2], (NTOK, TOP), jnp.float32, 0.25, 1.0)
    counts = _counts()
    lab_np = np.repeat(np.arange(EXPERTS), counts)
    lab = jnp.asarray(lab_np)
    rank = jnp.asarray(np.arange(NPER) - (np.cumsum(counts) - counts)[lab_np])

    def one(k):
        k1, k2, k3 = jax.random.split(k, 3)
        rows = jax.random.permutation(k1, TOKENS)
        cols = jax.random.permutation(k2, jnp.tile(jnp.arange(TOP), (TOKENS, 1)), axis=1, independent=True)
        relabel = jax.random.permutation(k3, EXPERTS)
        p = jnp.arange(NPER)
        m = rows[p % TOKENS] * TOP + cols[p % TOKENS, p // TOKENS]
        return jnp.full((EXPERTS, BOUND), NPER, jnp.int32).at[relabel[lab], rank].set(m.astype(jnp.int32))

    slots = jax.vmap(one)(jax.random.split(kp[3], GROUP)).reshape(GROUP * EXPERTS, BOUND)
    w1 = (jax.random.normal(kw[0], (EXPERTS, D, FF), jnp.float32) * D ** -0.5).astype(jnp.bfloat16)
    w3 = (jax.random.normal(kw[1], (EXPERTS, D, FF), jnp.float32) * D ** -0.5).astype(jnp.bfloat16)
    w2 = (jax.random.normal(kw[2], (EXPERTS, FF, D), jnp.float32) * FF ** -0.5).astype(jnp.bfloat16)
    return dict(x=x, slots=slots, gates=gates, w1=w1, w3=w3, w2=w2, dy=dy)


def reference(x, slots, gates, w1, w3, w2, dy):
    sl = slots.reshape(GROUP, EXPERTS * BOUND)
    src = jnp.arange(GROUP)[:, None]
    lab = jnp.broadcast_to(jnp.repeat(jnp.arange(EXPERTS), BOUND)[None, :], sl.shape)
    asg = jnp.where(sl < NPER, src * NPER + sl, NASG)
    expert = jnp.zeros((NASG + 1,), jnp.int32).at[asg.reshape(-1)].set(lab.reshape(-1).astype(jnp.int32))[:NASG]
    counts = jnp.zeros((EXPERTS,), jnp.int32).at[expert].add(1)
    order = jnp.argsort(expert, stable=True)
    padded = (counts + ROWS - 1) // ROWS * ROWS
    pend = jnp.cumsum(padded)
    pstart = pend - padded
    cstart = jnp.cumsum(counts) - counts
    se = expert[order]
    pos = pstart[se] + jnp.arange(NASG) - cstart[se]
    table = jnp.full((NBLK * ROWS,), NASG, jnp.int32).at[pos].set(order.astype(jnp.int32)).reshape(NBLK, ROWS)
    blk_e = jnp.minimum(jnp.searchsorted(pend, jnp.arange(NBLK) * ROWS, side='right'), EXPERTS - 1)
    gflat = gates.reshape(-1)

    def body(carry, item):
        y_acc, dx_acc, dg_acc, dw1, dw3, dw2 = carry
        ids, e = item
        valid = ids < NASG
        a_ids = jnp.where(valid, ids, 0)
        tok = a_ids // TOP
        vf = valid.astype(jnp.float32)
        xb = jnp.where(valid[:, None], x[tok], jnp.zeros((), x.dtype))
        g = gflat[a_ids] * vf
        a = jnp.dot(xb, w1[e], preferred_element_type=jnp.float32)
        b = jnp.dot(xb, w3[e], preferred_element_type=jnp.float32)
        sg = jax.nn.sigmoid(a)
        s = a * sg
        h = (s * b).astype(jnp.bfloat16)
        o = jnp.dot(h, w2[e], preferred_element_type=jnp.float32).astype(jnp.bfloat16)
        dyb = dy[tok].astype(jnp.float32)
        do = (g[:, None] * dyb).astype(jnp.bfloat16)
        dgb = jnp.sum(dyb * o.astype(jnp.float32), axis=1) * vf
        dh = jnp.dot(do, w2[e].T, preferred_element_type=jnp.float32)
        da = (dh * b * (sg * (1.0 + a * (1.0 - sg)))).astype(jnp.bfloat16)
        db = (dh * s).astype(jnp.bfloat16)
        dxb = (jnp.dot(da, w1[e].T, preferred_element_type=jnp.float32) + jnp.dot(db, w3[e].T, preferred_element_type=jnp.float32)).astype(jnp.bfloat16)
        y_acc = y_acc.at[tok].add(g[:, None] * o.astype(jnp.float32))
        dx_acc = dx_acc.at[tok].add(vf[:, None] * dxb.astype(jnp.float32))
        dg_acc = dg_acc.at[a_ids].add(dgb)
        dw1 = dw1.at[e].add(jnp.dot(xb.T, da, preferred_element_type=jnp.float32))
        dw3 = dw3.at[e].add(jnp.dot(xb.T, db, preferred_element_type=jnp.float32))
        dw2 = dw2.at[e].add(jnp.dot(h.T, do, preferred_element_type=jnp.float32))
        return (y_acc, dx_acc, dg_acc, dw1, dw3, dw2), None

    init = (jnp.zeros((NTOK, D), jnp.float32), jnp.zeros((NTOK, D), jnp.float32), jnp.zeros((NASG,), jnp.float32),
            jnp.zeros((EXPERTS, D, FF), jnp.float32), jnp.zeros((EXPERTS, D, FF), jnp.float32),
            jnp.zeros((EXPERTS, FF, D), jnp.float32))
    (y_acc, dx_acc, dg_acc, dw1, dw3, dw2), _ = lax.scan(body, init, (table, blk_e))
    return (y_acc.astype(jnp.bfloat16), dx_acc.astype(jnp.bfloat16), dg_acc.reshape(NTOK, TOP), dw1, dw3, dw2)
```

```python
import functools
import jax
import jax.numpy as jnp
from jax import lax
from jax.experimental import pallas as pl
from jax.experimental.pallas import tpu as pltpu
from jax.sharding import PartitionSpec as P

F32 = jnp.float32
BF16 = jnp.bfloat16


def _dot(a, b, ca, cb):
    return lax.dot_general(a, b, (((ca,), (cb,)), ((), ())), preferred_element_type=F32)


def _expert_kernel(tile, x_ref, do_ref, w1_ref, w3_ref, w2_ref, *rest):
    o_ref, dx_ref, dw1_ref, dw3_ref, dw2_ref, h_s, da_s, db_s = rest[-8:]
    n_o, _, cap, d = x_ref.shape
    rows = n_o * cap
    w1 = w1_ref[0]
    w3 = w3_ref[0]
    w2 = w2_ref[0]
    per = tile // cap
    for r in range(rows // tile):
        xs = x_ref[r * per:(r + 1) * per, 0].reshape(tile, d)
        dos = do_ref[r * per:(r + 1) * per, 0].reshape(tile, d)
        a = _dot(xs, w1, 1, 0)
        b = _dot(xs, w3, 1, 0)
        sg = jax.nn.sigmoid(a)
        s = a * sg
        h = (s * b).astype(BF16)
        dh = _dot(dos, w2, 1, 1)
        da = (dh * b * (sg * (1.0 + a * (1.0 - sg)))).astype(BF16)
        db = (dh * s).astype(BF16)
        h_s[r * tile:(r + 1) * tile] = h
        da_s[r * tile:(r + 1) * tile] = da
        db_s[r * tile:(r + 1) * tile] = db
        o_ref[r * per:(r + 1) * per, 0, 0] = _dot(h, w2, 1, 0).astype(BF16).reshape(per, cap, d)
        dx = _dot(da, w1, 1, 1) + _dot(db, w3, 1, 1)
        dx_ref[r * per:(r + 1) * per, 0, 0] = dx.astype(BF16).reshape(per, cap, d)
    xa = x_ref[:, 0].reshape(rows, d)
    doa = do_ref[:, 0].reshape(rows, d)
    dw1_ref[0] = _dot(xa, da_s[...], 0, 0)
    dw3_ref[0] = _dot(xa, db_s[...], 0, 0)
    dw2_ref[0] = _dot(h_s[...], doa, 0, 0)


def _experts(c, n_c, x, do, w1, w3, w2, carry):
    n_o, n_i, cap, d = x.shape
    f = w1.shape[2]
    rows = n_o * cap
    tok = pl.BlockSpec((n_o, 1, cap, d), lambda i: (0, i, 0, 0))
    wab = pl.BlockSpec((1, d, f), lambda i: (i, 0, 0))
    wc = pl.BlockSpec((1, f, d), lambda i: (i, 0, 0))
    back = pl.BlockSpec((n_o, 1, 1, cap, d), lambda i: (0, c, i, 0, 0))
    full = jax.ShapeDtypeStruct((n_o, n_c, n_i, cap, d), BF16)
    extra = [] if carry is None else [pl.BlockSpec(memory_space=pl.ANY)] * 2
    alias = {} if carry is None else {5: 0, 6: 1}
    args = (x, do, w1, w3, w2) + (() if carry is None else carry)

    return pl.pallas_call(
        functools.partial(_expert_kernel, 512),
        grid=(n_i,),
        in_specs=[tok, tok, wab, wab, wc] + extra,
        out_specs=[back, back, wab, wab, wc],
        out_shape=[full, full, jax.ShapeDtypeStruct((n_i, d, f), F32), jax.ShapeDtypeStruct((n_i, d, f), F32),
                   jax.ShapeDtypeStruct((n_i, f, d), F32)],
        scratch_shapes=[pltpu.VMEM((rows, f), BF16)] * 3,
        input_output_aliases=alias,
        compiler_params=pltpu.CompilerParams(vmem_limit_bytes=60 * 1024 * 1024),
        cost_estimate=pl.CostEstimate(flops=18 * n_i * rows * d * f, transcendentals=n_i * rows * f,
                                      bytes_accessed=n_i * (8 * rows * d + 18 * d * f)),
        name='experts%d' % c,
    )(*args)


def solution(mesh):
    n_i = mesh.shape['ei']
    n_o = mesh.shape['eo']
    tok = P(('dp', 'ei', 'eo'), None)
    wsp = P(('ei', 'eo'), None, None)
    dwsp = P(('dp', 'ei', 'eo'), None, None)

    def local(x, slots, gates, w1, w3, w2, dy):
        t, d = x.shape
        k = gates.shape[1]
        n_exp, cap = slots.shape
        nk = t * k
        n_c = n_exp // (n_i * n_o)
        sl = slots.reshape(n_i, n_o, n_c, cap).transpose(1, 2, 0, 3)
        flat = sl.reshape(-1)
        gs = jnp.where(flat < nk, gates.reshape(-1)[jnp.minimum(flat, nk - 1)], 0.0)
        gs = gs.reshape(n_o, n_c, n_i, cap)

        xs, dos, ws = [], [], []
        for c in range(n_c):
            idx = (jnp.minimum(sl[:, c], nk - 1) // k).reshape(-1)
            xb = x[idx].reshape(n_o, n_i, cap, d)
            xs.append(lax.all_to_all(xb, 'eo', 0, 0, tiled=True))
            dob = (gs[:, c].reshape(-1)[:, None] * dy[idx].astype(F32)).astype(BF16).reshape(n_o, n_i, cap, d)
            dos.append(lax.all_to_all(dob, 'eo', 0, 0, tiled=True))
            ws.append([lax.all_gather(w[c:c + 1], 'ei', axis=0, tiled=True) for w in (w1, w3, w2)])
        carry = None
        grads = []
        for c in range(n_c):
            o, dx, *dw = _experts(c, n_c, xs[c], dos[c], *ws[c], carry)
            carry = (o, dx)
            grads.append([lax.psum_scatter(g, 'ei', scatter_dimension=0, tiled=True) for g in dw])
        ob = lax.all_to_all(carry[0], 'eo', 0, 0, tiled=True).reshape(n_exp * cap, d)
        dxb = lax.all_to_all(carry[1], 'eo', 0, 0, tiled=True).reshape(n_exp * cap, d)

        pos = jnp.zeros((nk + 1,), jnp.int32).at[flat].set(jnp.arange(n_exp * cap, dtype=jnp.int32))[:nk].reshape(t, k)
        dyf = dy.astype(F32)
        y = 0.0
        dgs = []
        for j in range(k):
            oj = ob[pos[:, j]].astype(F32)
            y = y + gates[:, j:j + 1] * oj
            dgs.append(jnp.sum(dyf * oj, axis=1))
        dgates = jnp.stack(dgs, axis=1)
        dx = 0.0
        for j in range(k):
            dx = dx + dxb[pos[:, j]].astype(F32)
        dw1, dw3, dw2 = (jnp.concatenate([g[q] for g in grads], axis=0) for q in range(3))
        return y.astype(BF16), dx.astype(BF16), dgates, dw1, dw3, dw2

    return jax.shard_map(local, mesh=mesh, in_specs=(tok, tok, tok, wsp, wsp, wsp, tok),
                         out_specs=(tok, tok, tok, dwsp, dwsp, dwsp), check_vma=False)
```
